256 devices in a mesh: gx: 8 (over y, core), gy: 4 (over x), gz: 8 (over z).
Axes of the slice: x: 4, y: 4, z: 8, core: 2. Of those that a mesh axis runs over, the one named last changes fastest.
Arguments:
- leaf_coeffs: float32 [4096, 1000], P(('gx', 'gy', 'gz')), may hold values from -6 to 6
- operator_blocks: float32 [2, 7, 4, 3, 400], replicated, may hold values from -0.5 to 0.5
- term_ranks: int32 [2, 7], replicated, may hold values from 2 to 4
- target_device: int32 [512, 7, 1], P(('gx', 'gy', 'gz')), may hold values from 0 to 31; in each aligned block of 14 rows (0 to 13, 14 to 27, ..., all dimensions but the last counted through in order) at most 2 rows name the same one
- target_slot: int32 [512, 7], P(('gx', 'gy', 'gz')), may hold values from 0 to 1
- coarse_targets: int32 [96, 7], P(('gx', 'gy')), may hold values from 0 to 95
- parent_place: int32 [32, 16], P(('gx', 'gy')), may hold values from 0 to 23, as said below
Outputs:
- leaf_result: float32 [4096, 1000], P(('gx', 'gy', 'gz'))
The draws below stay inside these ranges and needn't reach their ends.
Inputs may be any that keep to these rules, and one draw needn't show every extreme that they name: `parent_place`: each row names distinct values. `target_device`: among the rows of one device, no value is named more than 2 times.
All inputs are finite; a program needn't handle non-finite values.
Results may differ from the reference program's by a relative error of at most 0.0003.
Values sent between devices are 32-bit elements; how exact they have to be, the bound alone decides.
No kernel may reach another device: no remote copies, remote signals or barrier semaphores. Data moves between devices by JAX's collectives and lax.ppermute only.
A program may use at most 64 MiB of HBM per device.

```python
import math
import jax
import jax.numpy as jnp
import numpy as np
from jax import lax

ORDER = 10
TERMS = 4
DISP = 7
NODES1 = 2
C0 = 3
COLUMNS = 32
COLUMN1 = 16
NODES_ALL = 512
LEAVES = 4096
NODES0_ALL = 96
CAP1 = 2
N_GY = 4
N_GZ = 8


def draw_parent_place(key, part):
    column_keys = jax.random.split(jax.random.fold_in(key, 17), COLUMNS)

    def one_column(column_key):
        return jax.random.permutation(column_key, C0 * 8)[:COLUMN1]
    return jax.vmap(one_column)(column_keys).astype(jnp.int32)


def touch_ends(array, stream_key, least, largest):
    longest = array.shape.index(max(array.shape))
    spots = []
    for shift in (0, 1):
        where = [jax.random.randint(jax.random.fold_in(stream_key, axis), (), 0, length) for axis, length in enumerate(array.shape)]
        where[longest] = (where[longest] + shift) % array.shape[longest]
        spots.append(tuple(where))
    return array.at[spots[0]].set(least).at[spots[1]].set(largest)


def levels(own_key, dims, pieces, smallest, largest):
    def one(dim, parts):
        heights = jax.random.uniform(jax.random.fold_in(jax.random.fold_in(own_key, 6), dim), (parts,), jnp.float32, smallest / len(pieces), largest / len(pieces))
        return jnp.repeat(jnp.exp(heights), dims[dim] // parts).reshape((-1,) + (1,) * (len(dims) - dim - 1))

    level = one(*pieces[0])
    for cut in pieces[1:]:
        level = level * one(*cut)
    return level


def assign_block(stream_key, own, number, rows, amount, top, reach, skew):
    sequence = jax.random.permutation(stream_key, amount)
    packed, usual = load_shares(amount, rows * top, reach, skew, True), load_shares(amount, rows * top, reach, skew, False)
    places = jnp.arange(amount)

    def named(tallies, turn):
        used = int((tallies > 0).sum())
        fixed = max(1, used // 4)
        shifted = fixed + (places - fixed + turn * (used - fixed)) % max(1, amount - fixed)
        return jnp.zeros((amount,), jnp.int32).at[sequence[jnp.where(places < fixed, places, shifted)]].set(jnp.asarray(tallies, jnp.int32))

    tallies = jnp.where(number % 4 == 0, named(packed, number // 4), named(usual, number - number // 4 - 1))
    mixed = jax.random.permutation(jax.random.fold_in(own, 3), amount)
    giver, taker = mixed[0:amount // 2 * 2:2], mixed[1:amount // 2 * 2:2]
    margin = jnp.minimum(tallies[giver] - 1, reach - tallies[taker]) // 2
    margin = jnp.where((giver == sequence[0]) | (taker == sequence[0]) | (tallies[taker] == 0), 0, jnp.maximum(margin, 0))
    shifted = jax.random.randint(jax.random.fold_in(own, 4), (amount // 2,), 0, 1 << 20) % (margin + 1)
    tallies = tallies.at[giver].add(-shifted).at[taker].add(shifted)
    members = jnp.searchsorted(jnp.cumsum(tallies), jnp.arange(rows * top), side="right").astype(jnp.int32)
    grid = members.reshape(top, rows).T
    grid = grid[jax.random.permutation(jax.random.fold_in(own, 1), rows)]
    turn = jax.random.randint(jax.random.fold_in(own, 2), (rows, 1), 0, top)
    return jnp.take_along_axis(grid, (jnp.arange(top)[None, :] + turn) % top, axis=1)


def load_shares(number_of, total, limit, lean, full):
    weights = [(1 << 20) // math.isqrt(rank ** lean) + 1 for rank in range(1, number_of + 1)]
    largest = limit if full else min(limit, max(-(-total // number_of), total * weights[0] // sum(weights)))
    least = 1 if total - largest >= number_of - 1 else 0
    holding, spare = [largest] + [least] * (number_of - 1), total - largest - least * (number_of - 1)
    while spare > 0:
        movable = [i for i in range(1, number_of) if holding[i] < largest] or [i for i in range(1, number_of) if holding[i] < limit]
        pool, budget = sum([weights[i] for i in movable]), spare
        for i in movable:
            addition = min(limit - holding[i], max(1, budget * weights[i] // pool), spare)
            holding[i] = holding[i] + addition
            spare = spare - addition
    return np.array(holding)


def normal_values(stream_key, dims, width, most, pieces=(), held_as=jnp.bfloat16):
    values = width * jax.random.normal(stream_key, dims, jnp.float32)
    if pieces:
        values = values * levels(stream_key, dims, pieces, -0.22, 0.18)
    return jnp.clip(values, -most, most).astype(held_as)


def setup_inputs(seed: int = 0) -> dict:
    keys = jax.random.split(jax.random.key(seed), 8)
    leaf_coeffs = normal_values(keys[0], (LEAVES, ORDER**3), 1.0, 6.0, ((0, 256),), jnp.float32)
    operator_blocks = normal_values(keys[1], (2, DISP, TERMS, 3, 4 * ORDER**2), (16 * ORDER) ** -0.5, 0.5, (), jnp.float32)
    term_ranks = touch_ends(jax.random.randint(keys[2], (2, DISP), TERMS // 2, TERMS + 1), jax.random.fold_in(keys[2], 1), TERMS // 2, TERMS).astype(jnp.int32)
    target_device_keys = jax.random.split(jax.random.fold_in(keys[3], 1), NODES_ALL * DISP // (NODES1 * DISP))
    target_device_turns = jax.random.permutation(jax.random.fold_in(keys[3], 3), NODES_ALL * DISP // (NODES1 * DISP))
    target_device = jax.vmap(lambda own, number: assign_block(jax.random.fold_in(keys[3], 2), own, number, NODES1 * DISP, N_GY * N_GZ, 1, CAP1, 2))(target_device_keys, target_device_turns).reshape((NODES_ALL, DISP, 1))
    target_slot = touch_ends(jax.random.randint(keys[4], (NODES_ALL, DISP), 0, NODES1), jax.random.fold_in(keys[4], 1), 0, NODES1 - 1).astype(jnp.int32)
    coarse_targets = touch_ends(jax.random.randint(keys[5], (NODES0_ALL, DISP), 0, NODES0_ALL), jax.random.fold_in(keys[5], 1), 0, NODES0_ALL - 1).astype(jnp.int32)
    parent_place = draw_parent_place(jax.random.fold_in(keys[7], 71), 0)
    return {"leaf_coeffs": leaf_coeffs, "operator_blocks": operator_blocks, "term_ranks": term_ranks, "target_device": target_device, "target_slot": target_slot, "coarse_targets": coarse_targets, "parent_place": parent_place}


precise = lax.Precision.HIGHEST

def two_scale(edge_len):
    row_index = jnp.arange(edge_len)[:, None].astype(jnp.float32)
    col_index = jnp.arange(edge_len)[None, :].astype(jnp.float32)
    filter_table = jnp.sqrt(2.0 / edge_len) * jnp.cos(jnp.pi * (col_index + 0.5) * row_index / edge_len)
    return jnp.where(row_index == 0, filter_table * jnp.sqrt(0.5), filter_table)

def transform(blocks, filter_table, inverse):
    if inverse:
        filter_table = filter_table.T
    return jnp.einsum('ix,jy,kz,nxyz->nijk', filter_table, filter_table, filter_table, blocks, precision=precise)

def assemble(leaf_rows, order_len):
    node_count = leaf_rows.shape[0] // 8
    shaped = leaf_rows.reshape(node_count, 2, 2, 2, order_len, order_len, order_len)
    return shaped.transpose(0, 1, 4, 2, 5, 3, 6).reshape(node_count, 2 * order_len, 2 * order_len, 2 * order_len)

def split_octants(blocks, order_len):
    node_count = blocks.shape[0]
    shaped = blocks.reshape(node_count, 2, order_len, 2, order_len, 2, order_len)
    return shaped.transpose(0, 1, 3, 5, 2, 4, 6).reshape(node_count * 8, order_len ** 3)

def displaced(blocks, matrices, rank_now):
    node_count, edge_len = (blocks.shape[0], blocks.shape[1])

    def per_term(running, entries):
        factors, term_index = entries
        flag = (term_index < rank_now).astype(jnp.float32)
        first_factor = factors[0].reshape(edge_len, edge_len) * flag
        second_factor = factors[1].reshape(edge_len, edge_len)
        third_factor = factors[2].reshape(edge_len, edge_len)
        partial_value = jnp.einsum('ia,nabc->nibc', first_factor, blocks, precision=precise)
        partial_value = jnp.einsum('jb,nibc->nijc', second_factor, partial_value, precision=precise)
        partial_value = jnp.einsum('kc,nijc->nijk', third_factor, partial_value, precision=precise)
        return (running + partial_value, None)
    term_index = jnp.arange(matrices.shape[0], dtype=jnp.int32)
    running, _ = lax.scan(per_term, jnp.zeros(blocks.shape, jnp.float32), (matrices, term_index))
    return running.reshape(node_count, edge_len ** 3)

def apply_level(blocks, matrices, ranks, targets, count):

    def per_disp(accumulated, entries):
        matrix_set, rank_now, target = entries
        return (accumulated.at[target].add(displaced(blocks, matrix_set, rank_now)), None)
    start = jnp.zeros((count, blocks.shape[1] ** 3), jnp.float32)
    accumulated, _ = lax.scan(per_disp, start, (matrices, ranks, targets.T))
    return accumulated

def reference(leaf_coeffs, operator_blocks, term_ranks, target_device, target_slot, coarse_targets, parent_place):
    edge_len = 2 * ORDER
    filter_table = two_scale(edge_len)
    node_count = leaf_coeffs.shape[0] // 8
    middle_blocks = transform(assemble(leaf_coeffs, ORDER), filter_table, False)
    corner_parts = middle_blocks[:, :ORDER, :ORDER, :ORDER].reshape(node_count, ORDER ** 3)
    column_count = parent_place.shape[0]
    row_index = (jnp.arange(column_count, dtype=jnp.int32)[:, None] * (8 * C0) + parent_place).reshape(-1).astype(jnp.int32)
    octants = jnp.zeros((column_count * C0 * 8, ORDER ** 3), jnp.float32).at[row_index].set(corner_parts)
    coarse_blocks = transform(assemble(octants, ORDER), filter_table, False)
    coarse_applied = apply_level(coarse_blocks, operator_blocks[0], term_ranks[0], coarse_targets, column_count * C0)
    coarse_back = split_octants(transform(coarse_applied.reshape(-1, edge_len, edge_len, edge_len), filter_table, True), ORDER)
    from_parent = coarse_back[row_index]
    slab_index = jnp.arange(node_count, dtype=jnp.int32) // (NODES1 * N_GY * N_GZ)
    middle_targets = slab_index[:, None] * (N_GY * N_GZ * NODES1) + target_device[:, :, 0] * NODES1 + target_slot
    middle_applied = apply_level(middle_blocks, operator_blocks[1], term_ranks[1], middle_targets.astype(jnp.int32), node_count)
    middle_total = middle_applied.reshape(node_count, edge_len, edge_len, edge_len)
    middle_total = middle_total.at[:, :ORDER, :ORDER, :ORDER].add(from_parent.reshape(node_count, ORDER, ORDER, ORDER))
    return split_octants(transform(middle_total, filter_table, True), ORDER)
```

```python
import jax
import jax.numpy as jnp
import numpy as np
from jax import lax
from jax.experimental import pallas as pl
from jax.experimental.pallas import tpu as pltpu
from jax.sharding import PartitionSpec as P

ORDER = 10
EDGE = 20
ZPAD = 24
LANES = 512
DISP = 7
TERMS = 4
SLOTS = 8
C0 = 3
NODES1 = 2
F32 = jnp.float32
BF16 = jnp.bfloat16


def _tables():
    n = EDGE
    i = np.arange(n)[:, None]
    x = np.arange(n)[None, :]
    h = np.sqrt(2.0 / n) * np.cos(np.pi * (x + 0.5) * i / n)
    h[0] *= np.sqrt(0.5)
    c = {}
    perm = np.zeros((LANES, LANES))
    for oy in range(2):
        for oz in range(2):
            for b in range(10):
                for k in range(10):
                    perm[(2 * oy + oz) * 128 + 10 * b + k, (10 * oy + b) * ZPAD + 10 * oz + k] = 1
    c["perm"] = perm
    c["permt"] = perm.T.copy()
    ra = np.zeros((4, 40, 160))
    rt = np.zeros((160, 160))
    for nn in range(2):
        for ox in range(2):
            for oyz in range(4):
                for a in range(10):
                    row = nn * 20 + ox * 10 + a
                    leaf = 8 * nn + 4 * ox + oyz
                    ra[oyz, row, a * 16 + leaf] = 1
                    rt[a * 16 + leaf, oyz * 40 + row] = 1
    c["ra"] = ra
    c["rt"] = rt
    hx = np.zeros((24, 40))
    ht = np.zeros((40, 24))
    for nn in range(2):
        for ii in range(10):
            for xx in range(20):
                hx[ii * 2 + nn, nn * 20 + xx] = h[ii, xx]
                ht[nn * 20 + xx, nn * 12 + ii] = h[ii, xx]
    c["hx"] = hx
    c["ht"] = ht
    hy = np.zeros((LANES, 128))
    for y in range(20):
        for z in range(20):
            hy[y * ZPAD + z, :100] = np.outer(h[:10, y], h[:10, z]).reshape(-1)
    c["hy"] = hy
    c["hyt"] = hy.T.copy()
    ca = np.zeros((24, 400))
    ci = np.zeros((24, 400))
    g0 = np.zeros((400, 160))
    g1 = np.zeros((400, LANES))
    g2 = np.zeros((400, LANES))
    for ii in range(20):
        for a in range(20):
            q = ii * 20 + a
            ca[:20, q] = h[a]
            ci[:20, q] = h[ii]
            g0[q] = np.repeat(h[a], SLOTS)
            for y in range(20):
                g1[q, y * ZPAD : y * ZPAD + 20] = h[ii, y]
                g2[q, y * ZPAD : y * ZPAD + 20] = h[ii]
    c["ca"], c["ci"], c["g0"], c["g1"], c["g2"] = ca, ci, g0, g1, g2
    po = np.zeros((160, 160))
    for xx in range(20):
        for r in range(8):
            po[(r // 2) * 40 + (r % 2) * 20 + xx, xx * 8 + r] = 1
    c["po"] = po
    out = {k: np.asarray(v, np.float32) for k, v in c.items()}
    return out


def _onehot(t):
    return jnp.asarray(t, BF16)


def _pair(t):
    t = np.asarray(t, np.float32)
    hi = t.astype(jnp.bfloat16)
    lo = (t - hi.astype(np.float32)).astype(jnp.bfloat16)
    return jnp.asarray(np.stack([hi, lo]))


def dot(a, b):
    return jnp.dot(a, b, preferred_element_type=F32)


def dot_nt(a, b):
    return lax.dot_general(a, b, (((1,), (1,)), ((), ())), preferred_element_type=F32)


def split2(v):
    hi = v.astype(BF16)
    return hi, (v - hi.astype(F32)).astype(BF16)


def split3(v):
    hi = v.astype(BF16)
    rest = v - hi.astype(F32)
    mid = rest.astype(BF16)
    return hi, mid, (rest - mid.astype(F32)).astype(BF16)


def dot3(a, b):
    ah, al = a
    bh, bl = b
    return dot(ah, bh) + (dot(al, bh) + dot(ah, bl))


def iota(shape, dim):
    return lax.broadcasted_iota(jnp.int32, shape, dim)


def pack_kernel(leaf, td, ts, ct, pp, ra, perm, hx, hy, wmsg, cmsg, rows):
    rows[...] = jnp.zeros_like(rows)
    for a in range(ORDER):
        rows[16 * a : 16 * a + 16, :100] = leaf[:, 100 * a : 100 * a + 100]
    w = jnp.zeros((40, LANES), F32)
    for part in split3(rows[...]):
        pieces = [dot(ra[o], part) for o in range(4)]
        w = w + dot(jnp.concatenate(pieces, axis=1).astype(BF16), perm[...])
    first = dot3((hx[0], hx[1]), split2(w))
    corner = dot3(split2(first), (hy[0], hy[1]))
    lane = iota((40, LANES), 1)
    row = iota((40, LANES), 0)
    for n in range(NODES1):
        mine = (row // EDGE) == n
        for e in range(DISP):
            w = jnp.where(mine & (lane == 480 + e), td[n, e].astype(F32), w)
            w = jnp.where(mine & (lane == 488 + e), ts[n, e].astype(F32), w)
    wmsg[...] = w
    z = lax.axis_index("gz")
    lane2 = iota((2, 128), 1)
    row2 = iota((2, 128), 0)
    head = corner[0:2, :]
    for n in range(NODES1):
        q = pp[0, z * NODES1 + n]
        head = jnp.where((row2 == n) & (lane2 == 108), (q % 8).astype(F32), head)
        for e in range(DISP):
            head = jnp.where((row2 == n) & (lane2 == 100 + e), ct[q // 8, e].astype(F32), head)
    cmsg[:, 0:128] = head
    for i in range(1, ORDER):
        cmsg[:, 128 * i : 128 * i + 128] = corner[2 * i : 2 * i + 2, :]


def prep_kernel(ob, ranks, ci, ca, g0, g1, g2, a0, l1, l2, q0, q1, q2):
    level = pl.program_id(0)
    for e in range(DISP):
        for t in range(TERMS):
            k = e * TERMS + t
            keep = (t < ranks[level, e]).astype(F32)
            q0[24 * k : 24 * k + 24, :] = ob[0, e, t, 0:1, :] * keep * ci[...]
            q1[24 * k : 24 * k + 24, :] = ob[0, e, t, 1:2, :] * ca[...]
            q2[24 * k : 24 * k + 24, :] = ob[0, e, t, 2:3, :] * ca[...]
    a0[0] = dot3(split2(q0[...]), (g0[0], g0[1]))
    l1[0] = dot3(split2(q1[...]), (g1[0], g1[1]))
    l2[0] = dot3(split2(q2[...]), (g2[0], g2[1]))


def images(source, a0, l1, l2, acc, kh, kl, bd):
    first = pl.program_id(0) == 0

    @pl.when(first)
    def _():
        acc[...] = jnp.zeros_like(acc)
        for t in range(TERMS):
            kh[t, 480:, :] = jnp.zeros((32, LANES), BF16)
            kl[t, 480:, :] = jnp.zeros((32, LANES), BF16)

    src = split2(source)
    same = ((iota((8, 160), 1) % 8) == iota((8, 160), 0)).astype(F32)
    total = acc[...]
    for t in range(TERMS):
        for i in range(EDGE):
            bd[t, 8 * i : 8 * i + 8, :] = a0[0, 24 * t + i : 24 * t + i + 1, :] * same
        third = l2[0, 24 * t : 24 * t + 24, :]
        for y in range(0, EDGE, 2):
            one = l1[0, 24 * t + y : 24 * t + y + 1, :] * third
            two = l1[0, 24 * t + y + 1 : 24 * t + y + 2, :] * third
            hi, lo = split2(jnp.concatenate([one, two], axis=0))
            kh[t, ZPAD * y : ZPAD * y + 48, :] = hi
            kl[t, ZPAD * y : ZPAD * y + 48, :] = lo
        mixed = split2(dot3(split2(bd[t]), src))
        total = total + dot3(mixed, (kh[t], kl[t]))
    acc[...] = total


def coarse_kernel(corners, pp, a0, l1, l2, perm, permt, out, acc, kh, kl, bd, gs, sw):
    e = pl.program_id(0)

    @pl.when(e == 0)
    def _():
        sel = (iota((16, 128), 1) == iota((16, 128), 0) + 100).astype(BF16)
        info = dot_nt(sel, corners[:, 0:128].astype(BF16))
        col = lax.axis_index("gx") * lax.axis_size("gy") + lax.axis_index("gy")
        r8 = iota((8, 64), 0)
        want = jnp.where(r8 < C0, (col * C0 + r8), -1).astype(F32)
        octant = info[8:9, :]
        blocks = []
        for oyz in range(4):
            for d in range(DISP):
                hit = info[d : d + 1, :] == want
                for ox in range(2):
                    there = octant == float(4 * ox + oyz)
                    blocks.append(jnp.where(hit & there, 1.0, 0.0))
        pick = jnp.concatenate(blocks, axis=0).astype(BF16)
        hi, lo = split2(corners[...])
        gs[...] = dot(pick, hi) + dot(pick, lo)

    for oyz in range(4):
        for ox in range(2):
            base = (oyz * DISP + e) * 16 + ox * 8
            for a in range(ORDER):
                sw[(ox * 10 + a) * 8 : (ox * 10 + a) * 8 + 8, 128 * oyz : 128 * oyz + 128] = gs[
                    pl.ds(base, 8), 128 * a : 128 * a + 128
                ]
    hi, lo = split2(sw[...])
    source = dot(hi, perm[...]) + dot(lo, perm[...])
    images(source, a0, l1, l2, acc, kh, kl, bd)

    @pl.when(e == DISP - 1)
    def _():
        col = iota((ZPAD, 640), 1)
        code = ((col % 8) * 4 + col // 160) * EDGE + (col % 160) // 8
        row = iota((ZPAD, 640), 0)
        a = row % 12
        blocks = []
        for z in range(8):
            qs = [pp[0, NODES1 * z + n] for n in range(NODES1)]
            bases = [((q // 8) * 4 + q % 4) * EDGE + ((q % 8) // 4) * ORDER for q in qs]
            base = jnp.where(row < 12, bases[0], bases[1])
            blocks.append(jnp.where((a < ORDER) & (code == base + a), 1.0, 0.0))
        pick = jnp.concatenate(blocks, axis=0).astype(BF16)
        picked = jnp.zeros((192, 128), F32)
        for part in split3(acc[...]):
            moved = dot(part, permt[...]).astype(BF16)
            stacked = jnp.concatenate([moved[:, 128 * o : 128 * o + 128] for o in range(4)], axis=0)
            picked = picked + dot(pick, stacked)
        for z in range(8):
            out[z] = picked[ZPAD * z : ZPAD * z + ZPAD, :]


def middle_kernel(wall, a0, l1, l2, po, out, acc, kh, kl, bd, info):
    e = pl.program_id(0)

    @pl.when(e == 0)
    def _():
        sel = (iota((16, 128), 1) == iota((16, 128), 0) + 96).astype(BF16)
        raw = dot_nt(sel, wall[:, 384:512].astype(BF16))
        device = raw[0:8, :]
        gy = jnp.floor(device * 0.125)
        gz = device - gy * 8.0
        z = lax.axis_index("gz").astype(F32)
        info[...] = jnp.where(gz == z, gy * 2.0 + raw[8:16, :], -1.0)

    lane = iota((160, 320), 1)
    row = iota((160, 320), 0)
    target = info[pl.ds(e, 1), :]
    hit = (lane % EDGE == row // 8) & (target == (row % 8).astype(F32))
    pick = jnp.where(hit, 1.0, 0.0).astype(BF16)
    hi, lo = split2(wall[...])
    source = dot(pick, hi) + dot(pick, lo)
    images(source, a0, l1, l2, acc, kh, kl, bd)

    @pl.when(e == DISP - 1)
    def _():
        moved = jnp.zeros((160, LANES), F32)
        for part in split3(acc[...]):
            moved = moved + dot(po[...], part)
        for g in range(4):
            out[g] = moved[40 * g : 40 * g + 40, :]


def final_kernel(mid, coarse, ht, hyt, permt, rt, out):
    total = (mid[0] + mid[1]) + (mid[2] + mid[3])
    corner = coarse[0]
    for z in range(1, 8):
        corner = corner + coarse[z]
    up = dot3((ht[0], ht[1]), split2(corner))
    total = total + dot3(split2(up), (hyt[0], hyt[1]))
    rows = jnp.zeros((160, 128), F32)
    for part in split3(total):
        moved = dot(part, permt[...]).astype(BF16)
        stacked = jnp.concatenate([moved[:, 128 * o : 128 * o + 128] for o in range(4)], axis=0)
        rows = rows + dot(rt[...], stacked)
    for a in range(ORDER):
        out[:, 100 * a : 100 * a + 100] = rows[16 * a : 16 * a + 16, :100]


VM = pl.BlockSpec(memory_space=pltpu.MemorySpace.VMEM)
SM = pl.BlockSpec(memory_space=pltpu.MemorySpace.SMEM)
INTERPRET = False


def sds(*shape):
    return jax.ShapeDtypeStruct(shape, F32)


def _params():
    return pltpu.CompilerParams(vmem_limit_bytes=56 * 1024 * 1024)


def level_specs():
    def of(rows, lanes):
        return pl.BlockSpec((1, rows, lanes), lambda e: (0, e, 0))

    return [of(96, 160), of(96, LANES), of(96, LANES)]


def level_scratch():
    return [
        pltpu.VMEM((160, LANES), F32),
        pltpu.VMEM((TERMS, LANES, LANES), BF16),
        pltpu.VMEM((TERMS, LANES, LANES), BF16),
        pltpu.VMEM((TERMS, 160, 160), F32),
    ]


def const(shape):
    return pl.BlockSpec(shape, lambda *_: (0,) * len(shape))


def gather_rows(value, axis):
    copies = jnp.broadcast_to(value, (lax.axis_size(axis), *value.shape))
    return lax.all_to_all(copies, axis, split_axis=0, concat_axis=0, tiled=True)


def on_device(leaf, ob, ranks, td, ts, ct, pp):
    c = _tables()
    perm, permt = _onehot(c["perm"]), _onehot(c["permt"])
    wmsg, cmsg = pl.pallas_call(
        pack_kernel,
        out_shape=(sds(40, LANES), sds(2, 1280)),
        in_specs=[VM, SM, SM, SM, SM, VM, VM, VM, VM],
        out_specs=(VM, VM),
        scratch_shapes=[pltpu.VMEM((160, 128), F32)],
        compiler_params=_params(),
        interpret=INTERPRET,
        name="pack",
    )(
        leaf,
        td.reshape(NODES1, DISP),
        ts,
        ct,
        pp,
        _onehot(c["ra"]),
        perm,
        _pair(c["hx"]),
        _pair(c["hy"]),
    )
    corners = gather_rows(cmsg, ("gx", "gy")).reshape(64, 1280)
    wall = gather_rows(wmsg, "gz").reshape(320, LANES)
    rows = DISP * TERMS * 24
    mats = pl.pallas_call(
        prep_kernel,
        grid=(2,),
        out_shape=(sds(2, rows, 160), sds(2, rows, LANES), sds(2, rows, LANES)),
        in_specs=[
            pl.BlockSpec((1, DISP, TERMS, 3, 400), lambda l: (l, 0, 0, 0, 0)),
            SM,
            const((24, 400)),
            const((24, 400)),
            const((2, 400, 160)),
            const((2, 400, LANES)),
            const((2, 400, LANES)),
        ],
        out_specs=tuple(
            pl.BlockSpec((1, rows, n), lambda l: (l, 0, 0)) for n in (160, LANES, LANES)
        ),
        scratch_shapes=[pltpu.VMEM((rows, 400), F32)] * 3,
        compiler_params=_params(),
        interpret=INTERPRET,
        name="prep",
    )(
        ob,
        ranks,
        jnp.asarray(c["ci"]),
        jnp.asarray(c["ca"]),
        _pair(c["g0"]),
        _pair(c["g1"]),
        _pair(c["g2"]),
    )

    def specs(level):
        def of(lanes):
            return pl.BlockSpec((1, 96, lanes), lambda e: (level, e, 0))

        return [of(160), of(LANES), of(LANES)]

    coarse = pl.pallas_call(
        coarse_kernel,
        grid=(DISP,),
        out_shape=sds(8, 24, 128),
        in_specs=[
            const((64, 1280)),
            SM,
            *specs(0),
            const((LANES, LANES)),
            const((LANES, LANES)),
        ],
        out_specs=const((8, 24, 128)),
        scratch_shapes=[
            *level_scratch(),
            pltpu.VMEM((448, 1280), F32),
            pltpu.VMEM((160, LANES), F32),
        ],
        compiler_params=_params(),
        interpret=INTERPRET,
        name="coarse",
    )(corners, pp, *mats, perm, permt)
    middle = pl.pallas_call(
        middle_kernel,
        grid=(DISP,),
        out_shape=sds(4, 40, LANES),
        in_specs=[const((320, LANES)), *specs(1), const((160, 160))],
        out_specs=const((4, 40, LANES)),
        scratch_shapes=[*level_scratch(), pltpu.VMEM((8, 320), F32)],
        compiler_params=_params(),
        interpret=INTERPRET,
        name="middle",
    )(wall, *mats, _onehot(c["po"]))
    coarse = lax.all_to_all(coarse, "gz", split_axis=0, concat_axis=0, tiled=True)
    middle = lax.all_to_all(middle, "gy", split_axis=0, concat_axis=0, tiled=True)
    return pl.pallas_call(
        final_kernel,
        out_shape=sds(16, 1000),
        in_specs=[VM] * 6,
        out_specs=VM,
        compiler_params=_params(),
        interpret=INTERPRET,
        name="final",
    )(middle, coarse, _pair(c["ht"]), _pair(c["hyt"]), permt, _onehot(c["rt"]))


def solution(mesh):
    in_specs = (
        P(("gx", "gy", "gz"), None),
        P(),
        P(),
        P(("gx", "gy", "gz"), None, None),
        P(("gx", "gy", "gz"), None),
        P(("gx", "gy"), None),
        P(("gx", "gy"), None),
    )
    out_specs = P(("gx", "gy", "gz"), None)
    return jax.shard_map(
        on_device, mesh=mesh, in_specs=in_specs, out_specs=out_specs, check_vma=False
    )
```

```python
import jax
import jax.numpy as jnp
import numpy as np
from jax import lax
from jax.experimental import pallas as pl
from jax.experimental.pallas import tpu as pltpu
from jax.sharding import PartitionSpec as P

ORDER = 10
EDGE = 20
ZPAD = 24
LANES = 512
DISP = 7
TERMS = 4
SLOTS = 8
C0 = 3
NODES1 = 2
F32 = jnp.float32
BF16 = jnp.bfloat16


def _tables():
    n = EDGE
    i = np.arange(n)[:, None]
    x = np.arange(n)[None, :]
    h = np.sqrt(2.0 / n) * np.cos(np.pi * (x + 0.5) * i / n)
    h[0] *= np.sqrt(0.5)
    c = {}
    lanes = np.full((8, LANES), -1)
    for y in range(EDGE):
        for z in range(EDGE):
            at = (2 * (y // 10) + z // 10) * 128 + (y % 10) * 10 + z % 10
            lanes[0, y * ZPAD + z] = at
            lanes[1, at] = y * ZPAD + z
    c["lanes"] = lanes
    ra = np.zeros((4, 40, 160))
    rt = np.zeros((160, 160))
    for nn in range(2):
        for ox in range(2):
            for oyz in range(4):
                for a in range(10):
                    row = nn * 20 + ox * 10 + a
                    leaf = 8 * nn + 4 * ox + oyz
                    ra[oyz, row, a * 16 + leaf] = 1
                    rt[a * 16 + leaf, oyz * 40 + row] = 1
    c["ra"] = ra
    c["rt"] = rt
    hx = np.zeros((24, 40))
    ht = np.zeros((40, 24))
    for nn in range(2):
        for ii in range(10):
            for xx in range(20):
                hx[ii * 2 + nn, nn * 20 + xx] = h[ii, xx]
                ht[nn * 20 + xx, nn * 12 + ii] = h[ii, xx]
    c["hx"] = hx
    c["ht"] = ht
    hy = np.zeros((LANES, 128))
    for y in range(20):
        for z in range(20):
            hy[y * ZPAD + z, :100] = np.outer(h[:10, y], h[:10, z]).reshape(-1)
    c["hy"] = hy
    c["hyt"] = hy.T.copy()
    ca = np.zeros((24, 400))
    ci = np.zeros((24, 400))
    folds = np.zeros((2, 400, 128))
    wide = np.zeros((3, 32, LANES))
    for ii in range(20):
        for a in range(20):
            q = ii * 20 + a
            ca[:20, q] = h[a]
            ci[:20, q] = h[ii]
            for k in range(3):
                folds[0, q, 32 * k + a] = 1
                folds[1, q, 32 * k + ii] = 1
        for k in range(3):
            wide[0, ii, 80 * k : 80 * k + 80] = np.repeat(h[ii], 4)
        for y in range(20):
            wide[1, ii, y * ZPAD : y * ZPAD + 20] = h[ii, y]
            wide[2, ii, y * ZPAD : y * ZPAD + 20] = h[ii]
    high = np.asarray(np.asarray(wide, np.float32).astype(jnp.bfloat16), np.float32)
    c["wide"] = np.concatenate([high, high, wide - high, np.zeros((3, 32, LANES))], axis=1)
    c["ca"], c["ci"], c["folds"] = ca, ci, folds
    po = np.zeros((160, 160))
    for xx in range(20):
        for r in range(8):
            po[(r // 2) * 40 + (r % 2) * 20 + xx, (r // 4) * 80 + xx * 4 + r % 4] = 1
    c["po"] = po
    return c


def _onehot(t):
    return jnp.asarray(t, BF16)


def _pair(t):
    t = np.asarray(t, np.float32)
    hi = t.astype(jnp.bfloat16)
    lo = (t - hi.astype(np.float32)).astype(jnp.bfloat16)
    return jnp.asarray(np.stack([hi, lo]))


def dot(a, b):
    return jnp.dot(a, b, preferred_element_type=F32)


def dot_nt(a, b):
    return lax.dot_general(a, b, (((1,), (1,)), ((), ())), preferred_element_type=F32)


def split2(v):
    hi = v.astype(BF16)
    return hi, (v - hi.astype(F32)).astype(BF16)


def split3(v):
    hi = v.astype(BF16)
    rest = v - hi.astype(F32)
    mid = rest.astype(BF16)
    return hi, mid, (rest - mid.astype(F32)).astype(BF16)


def dot3(a, b):
    ah, al = a
    bh, bl = b
    return dot(ah, bh) + (dot(al, bh) + dot(ah, bl))


def iota(shape, dim):
    return lax.broadcasted_iota(jnp.int32, shape, dim)


def placed(lanes):
    return (iota((LANES, LANES), 0) == lanes).astype(F32).astype(BF16)


def pack_kernel(leaf, td, ts, ct, pp, lanes, ra, hx, hy, wmsg, cmsg, rows):
    perm = placed(lanes[0:1, :])
    rows[...] = jnp.zeros_like(rows)
    for a in range(ORDER):
        rows[16 * a : 16 * a + 16, :100] = leaf[:, 100 * a : 100 * a + 100]
    w = jnp.zeros((40, LANES), F32)
    for part in split3(rows[...]):
        pieces = [dot(ra[o], part) for o in range(4)]
        w = w + dot(jnp.concatenate(pieces, axis=1).astype(BF16), perm)
    first = dot3((hx[0], hx[1]), split2(w))
    corner = dot3(split2(first), (hy[0], hy[1]))
    lane = iota((40, LANES), 1)
    row = iota((40, LANES), 0)
    for n in range(NODES1):
        mine = (row // EDGE) == n
        for e in range(DISP):
            w = jnp.where(mine & (lane == 480 + e), td[n, e].astype(F32), w)
            w = jnp.where(mine & (lane == 488 + e), ts[n, e].astype(F32), w)
    for k in range(8):
        wmsg[k] = w
    z = lax.axis_index("gz")
    lane2 = iota((24, 128), 1)
    row2 = iota((24, 128), 0)
    for n in range(NODES1):
        q = pp[0, z * NODES1 + n]
        corner = jnp.where((row2 == n) & (lane2 == 108), (q % 8).astype(F32), corner)
        for e in range(DISP):
            here = (row2 == n) & (lane2 == 100 + e)
            corner = jnp.where(here, ct[q // 8, e].astype(F32), corner)
    for k in range(32):
        cmsg[k] = corner


def prep_kernel(ob, ranks, ci, ca, folds, wide, a0, l1, l2, q0, q1, q2):
    level = pl.program_id(0)
    for e in range(DISP):
        for t in range(TERMS):
            k = e * TERMS + t
            keep = (t < ranks[level, e]).astype(F32)
            q0[24 * k : 24 * k + 24, :] = ob[0, e, t, 0:1, :] * keep * ci[...]
            q1[24 * k : 24 * k + 24, :] = ob[0, e, t, 1:2, :] * ca[...]
            q2[24 * k : 24 * k + 24, :] = ob[0, e, t, 2:3, :] * ca[...]

    def folded(q, fold, d):
        hi, lo = split2(q[...])
        both = dot(hi, fold) + dot(lo, fold)
        lane = iota(both.shape, 1) // 32
        rest = both - both.astype(BF16).astype(F32)
        return dot(jnp.where(lane == 1, rest, both).astype(BF16), wide[d])

    a0[0] = folded(q0, folds[0], 0)[:, :256]
    l1[0] = folded(q1, folds[1], 1)
    l2[0] = folded(q2, folds[1], 2)


def images(rank, sources, a0, l1, l2, acc, kh, kl, bd):
    @pl.when(pl.program_id(0) == 0)
    def _():
        acc[...] = jnp.zeros_like(acc)
        for t in range(TERMS):
            kh[t, 480:, :] = jnp.zeros((32, LANES), BF16)
            kl[t, 480:, :] = jnp.zeros((32, LANES), BF16)

    lane = iota((8, 256), 1)
    row = iota((8, 256), 0)
    same = jnp.where((lane % 4 == row % 4) & (lane < 240), 1.0, 0.0)
    for t in range(TERMS):
        for i in range(0, EDGE, 2):
            at = 24 * t + i
            value = jnp.where(row < 4, a0[0, at : at + 1, :], a0[0, at + 1 : at + 2, :]) * same
            rest = value - value.astype(BF16).astype(F32)
            bd[80 * t + 4 * i : 80 * t + 4 * i + 8, :] = jnp.where(lane < 160, value, rest)
    left = bd[...].astype(BF16)
    zero = jnp.zeros((16, LANES), BF16)
    mixed = []
    for source in sources:
        hi, lo = split2(source)
        mixed.append(dot(left, jnp.concatenate([hi, lo, hi, zero], axis=0)))

    def build(t):
        third = l2[0, 24 * t : 24 * t + 24, :]
        for y in range(0, EDGE, 2):
            one = l1[0, 24 * t + y : 24 * t + y + 1, :] * third
            two = l1[0, 24 * t + y + 1 : 24 * t + y + 2, :] * third
            hi, lo = split2(jnp.concatenate([one, two], axis=0))
            kh[t, ZPAD * y : ZPAD * y + 48, :] = hi
            kl[t, ZPAD * y : ZPAD * y + 48, :] = lo

    def term(t):
        rows = [m[80 * t : 80 * t + 80, :] for m in mixed]
        both = split2(rows[0] if len(rows) == 1 else jnp.concatenate(rows, axis=0))
        return dot3(both, (kh[t], kl[t]))

    build(0)
    build(1)
    acc[...] = acc[...] + (term(0) + term(1))
    for t in range(2, TERMS):

        @pl.when(rank > t)
        def _():
            build(t)
            acc[...] = acc[...] + term(t)


def coarse_kernel(corners, pp, ranks, a0, l1, l2, lanes, out, acc, kh, kl, bd, gs, sw, perm):
    e = pl.program_id(0)

    @pl.when(e == 0)
    def _():
        perm[...] = placed(lanes[0:1, :])
        parts = []
        for a in range(ORDER):
            pair = [corners[pl.ds(2 * a + n, 32, stride=24), :] for n in range(NODES1)]
            parts.append(jnp.concatenate(pair, axis=0))
        value = jnp.concatenate(parts, axis=1)
        sel = (iota((16, 128), 1) == iota((16, 128), 0) + 100).astype(F32).astype(BF16)
        info = dot_nt(sel, value[:, 0:128].astype(BF16))
        col = lax.axis_index("gx") * lax.axis_size("gy") + lax.axis_index("gy")
        r4 = iota((8, 64), 0) % 4
        want = jnp.where(r4 < C0, (col * C0 + r4), -1).astype(F32)
        octant = info[8:9, :]
        blocks = []
        for oyz in range(4):
            for d in range(DISP):
                hit = info[d : d + 1, :] == want
                for ox in range(2):
                    there = octant == float(4 * ox + oyz)
                    blocks.append(jnp.where(hit & there, 1.0, 0.0))
        pick = jnp.concatenate(blocks, axis=0).astype(BF16)
        hi, lo = split2(value)
        gs[...] = dot(pick, hi) + dot(pick, lo)

    half = iota((8, 128), 0) < 4
    for oyz in range(4):
        for ox in range(2):
            base = (oyz * DISP + e) * 16 + ox * 8
            for a in range(0, ORDER, 2):
                one = gs[pl.ds(base, 8), 128 * a : 128 * a + 128]
                two = gs[pl.ds(base, 8), 128 * a + 128 : 128 * a + 256]
                at = (ox * 10 + a) * 4
                sw[at : at + 8, 128 * oyz : 128 * oyz + 128] = jnp.where(half, one, two)
    hi, lo = split2(sw[...])
    source = dot(hi, perm[...]) + dot(lo, perm[...])
    images(ranks[0, e], [source], a0, l1, l2, acc, kh, kl, bd)

    @pl.when(e == DISP - 1)
    def _():
        back = placed(lanes[1:2, :])
        col = iota((ZPAD, 320), 1)
        code = ((col % 4) * 4 + col // 80) * EDGE + (col % 80) // 4
        row = iota((ZPAD, 320), 0)
        a = row % 12
        blocks = []
        for z in range(8):
            qs = [pp[0, NODES1 * z + n] for n in range(NODES1)]
            bases = [((q // 8) * 4 + q % 4) * EDGE + ((q % 8) // 4) * ORDER for q in qs]
            base = jnp.where(row < 12, bases[0], bases[1])
            blocks.append(jnp.where((a < ORDER) & (code == base + a), 1.0, 0.0))
        pick = jnp.concatenate(blocks, axis=0).astype(BF16)
        picked = jnp.zeros((192, 128), F32)
        for part in split3(acc[...]):
            moved = dot(part, back).astype(BF16)
            stacked = jnp.concatenate([moved[:, 128 * o : 128 * o + 128] for o in range(4)], axis=0)
            picked = picked + dot(pick, stacked)
        for z in range(8):
            out[z] = picked[ZPAD * z : ZPAD * z + ZPAD, :]


def middle_kernel(wall, ranks, a0, l1, l2, po, out, acc, kh, kl, bd, info, wsplit):
    e = pl.program_id(0)

    @pl.when(e == 0)
    def _():
        sel = (iota((16, 128), 1) == iota((16, 128), 0) + 96).astype(F32).astype(BF16)
        raw = dot_nt(sel, wall[:, 384:512].astype(BF16))
        device = raw[0:8, :]
        gy = jnp.floor(device * 0.125)
        gz = device - gy * 8.0
        z = lax.axis_index("gz").astype(F32)
        info[...] = jnp.where(gz == z, gy * 2.0 + raw[8:16, :], -1.0)
        hi, lo = split2(wall[...])
        wsplit[0] = hi
        wsplit[1] = lo

    lane = iota((160, 320), 1)
    row = iota((160, 320), 0)
    slot = (row // 80) * 4 + row % 4
    target = info[pl.ds(e, 1), :]
    hit = (lane % EDGE == (row % 80) // 4) & (target == slot.astype(F32))
    pick = jnp.where(hit, 1.0, 0.0).astype(BF16)
    source = dot(pick, wsplit[0]) + dot(pick, wsplit[1])
    images(ranks[1, e], [source[:80, :], source[80:, :]], a0, l1, l2, acc, kh, kl, bd)

    @pl.when(e == DISP - 1)
    def _():
        moved = jnp.zeros((160, LANES), F32)
        for part in split3(acc[...]):
            moved = moved + dot(po[...], part)
        for g in range(4):
            out[g] = moved[40 * g : 40 * g + 40, :]


def final_kernel(mid, coarse, lanes, ht, hyt, rt, out):
    back = placed(lanes[1:2, :])
    total = (mid[0] + mid[1]) + (mid[2] + mid[3])
    corner = coarse[0]
    for z in range(1, 8):
        corner = corner + coarse[z]
    up = dot3((ht[0], ht[1]), split2(corner))
    total = total + dot3(split2(up), (hyt[0], hyt[1]))
    rows = jnp.zeros((160, 128), F32)
    for part in split3(total):
        moved = dot(part, back).astype(BF16)
        stacked = jnp.concatenate([moved[:, 128 * o : 128 * o + 128] for o in range(4)], axis=0)
        rows = rows + dot(rt[...], stacked)
    for a in range(ORDER):
        out[:, 100 * a : 100 * a + 100] = rows[16 * a : 16 * a + 16, :100]


VM = pl.BlockSpec(memory_space=pltpu.MemorySpace.VMEM)
SM = pl.BlockSpec(memory_space=pltpu.MemorySpace.SMEM)
COST = pl.CostEstimate(flops=8_000_000_000, transcendentals=0, bytes_accessed=4_000_000)


def sds(*shape):
    return jax.ShapeDtypeStruct(shape, F32)


def _params():
    return pltpu.CompilerParams(vmem_limit_bytes=56 * 1024 * 1024)


def level_scratch(rows):
    return [
        pltpu.VMEM((rows, LANES), F32),
        pltpu.VMEM((TERMS, LANES, LANES), BF16),
        pltpu.VMEM((TERMS, LANES, LANES), BF16),
        pltpu.VMEM((TERMS * 80, 256), F32),
    ]


def const(shape):
    return pl.BlockSpec(shape, lambda *_: (0,) * len(shape))


def swap(value, axis):
    return lax.all_to_all(value, axis, split_axis=0, concat_axis=0, tiled=True)


def on_device(leaf, ob, ranks, td, ts, ct, pp):
    c = _tables()
    lanes = jnp.asarray(c["lanes"], jnp.int32)
    wmsg, cmsg = pl.pallas_call(
        pack_kernel,
        out_shape=(sds(8, 40, LANES), sds(32, 24, 128)),
        in_specs=[VM, SM, SM, SM, SM, VM, VM, VM, VM],
        out_specs=(VM, VM),
        scratch_shapes=[pltpu.VMEM((160, 128), F32)],
        compiler_params=_params(),
        name="pack",
    )(
        leaf,
        td.reshape(NODES1, DISP),
        ts,
        ct,
        pp,
        lanes,
        _onehot(c["ra"]),
        _pair(c["hx"]),
        _pair(c["hy"]),
    )
    corners = swap(cmsg, ("gx", "gy")).reshape(768, 128)
    rows = DISP * TERMS * 24
    mats = pl.pallas_call(
        prep_kernel,
        grid=(2,),
        out_shape=(sds(2, rows, 256), sds(2, rows, LANES), sds(2, rows, LANES)),
        in_specs=[
            pl.BlockSpec((1, DISP, TERMS, 3, 400), lambda l: (l, 0, 0, 0, 0)),
            SM,
            const((24, 400)),
            const((24, 400)),
            const((2, 400, 128)),
            const((3, 128, LANES)),
        ],
        out_specs=tuple(
            pl.BlockSpec((1, rows, n), lambda l: (l, 0, 0)) for n in (256, LANES, LANES)
        ),
        scratch_shapes=[pltpu.VMEM((rows, 400), F32)] * 3,
        compiler_params=_params(),
        cost_estimate=COST,
        name="prep",
    )(ob, ranks, jnp.asarray(c["ci"]), jnp.asarray(c["ca"]), _onehot(c["folds"]), _onehot(c["wide"]))
    wmsg, *mats = lax.optimization_barrier((wmsg, *mats))
    wall = swap(wmsg, "gz").reshape(320, LANES)

    def specs(level):
        def of(lanes):
            return pl.BlockSpec((1, 96, lanes), lambda e: (level, e, 0))

        return [of(256), of(LANES), of(LANES)]

    coarse = pl.pallas_call(
        coarse_kernel,
        grid=(DISP,),
        out_shape=sds(8, 24, 128),
        in_specs=[const((768, 128)), SM, SM, *specs(0), const((8, LANES))],
        out_specs=const((8, 24, 128)),
        scratch_shapes=[
            *level_scratch(80),
            pltpu.VMEM((448, 1280), F32),
            pltpu.VMEM((80, LANES), F32),
            pltpu.VMEM((LANES, LANES), BF16),
        ],
        compiler_params=_params(),
        cost_estimate=COST,
        name="coarse",
    )(corners, pp, ranks, *mats, lanes)
    middle = pl.pallas_call(
        middle_kernel,
        grid=(DISP,),
        out_shape=sds(4, 40, LANES),
        in_specs=[const((320, LANES)), SM, *specs(1), const((160, 160))],
        out_specs=const((4, 40, LANES)),
        scratch_shapes=[
            *level_scratch(160),
            pltpu.VMEM((8, 320), F32),
            pltpu.VMEM((2, 320, LANES), BF16),
        ],
        compiler_params=_params(),
        cost_estimate=COST,
        name="middle",
    )(wall, ranks, *mats, _onehot(c["po"]))
    coarse = swap(coarse, "gz")
    middle = swap(middle, "gy")
    return pl.pallas_call(
        final_kernel,
        out_shape=sds(16, 1000),
        in_specs=[VM] * 6,
        out_specs=VM,
        compiler_params=_params(),
        name="final",
    )(middle, coarse, lanes, _pair(c["ht"]), _pair(c["hyt"]), _onehot(c["rt"]))


def solution(mesh):
    in_specs = (
        P(("gx", "gy", "gz"), None),
        P(),
        P(),
        P(("gx", "gy", "gz"), None, None),
        P(("gx", "gy", "gz"), None),
        P(("gx", "gy"), None),
        P(("gx", "gy"), None),
    )
    out_specs = P(("gx", "gy", "gz"), None)
    return jax.shard_map(
        on_device, mesh=mesh, in_specs=in_specs, out_specs=out_specs, check_vma=False
    )
```

```python
import jax
import jax.numpy as jnp
import numpy as np
from jax import lax
from jax.experimental import pallas as pl
from jax.experimental.pallas import tpu as pltpu
from jax.sharding import PartitionSpec as P

ORDER = 10
EDGE = 20
ZPAD = 24
LANES = 512
DISP = 7
TERMS = 4
SLOTS = 8
C0 = 3
NODES1 = 2
PAIRS = DISP * TERMS
F32 = jnp.float32
BF16 = jnp.bfloat16


def _tables():
    n = EDGE
    i = np.arange(n)[:, None]
    x = np.arange(n)[None, :]
    h = np.sqrt(2.0 / n) * np.cos(np.pi * (x + 0.5) * i / n)
    h[0] *= np.sqrt(0.5)
    c = {}
    lanes = np.full((8, LANES), -1)
    for y in range(EDGE):
        for z in range(EDGE):
            at = (2 * (y // 10) + z // 10) * 128 + (y % 10) * 10 + z % 10
            lanes[0, y * ZPAD + z] = at
            lanes[1, at] = y * ZPAD + z
    c["lanes"] = lanes
    ra = np.zeros((4, 40, 160))
    rt = np.zeros((160, 160))
    for nn in range(2):
        for ox in range(2):
            for oyz in range(4):
                for a in range(10):
                    row = nn * 20 + ox * 10 + a
                    leaf = 8 * nn + 4 * ox + oyz
                    ra[oyz, row, a * 16 + leaf] = 1
                    rt[a * 16 + leaf, oyz * 40 + row] = 1
    c["ra"] = ra
    c["rt"] = rt
    hx = np.zeros((24, 40))
    ht = np.zeros((40, 24))
    for nn in range(2):
        for ii in range(10):
            for xx in range(20):
                hx[ii * 2 + nn, nn * 20 + xx] = h[ii, xx]
                ht[nn * 20 + xx, nn * 12 + ii] = h[ii, xx]
    c["hx"] = hx
    c["ht"] = ht
    hy = np.zeros((LANES, 128))
    for y in range(20):
        for z in range(20):
            hy[y * ZPAD + z, :100] = np.outer(h[:10, y], h[:10, z]).reshape(-1)
    c["hy"] = hy
    c["hyt"] = hy.T.copy()
    ca = np.zeros((24, 400))
    ci = np.zeros((24, 400))
    folds = np.zeros((2, 400, 128))
    wide = np.zeros((3, 32, LANES))
    for ii in range(20):
        for a in range(20):
            q = ii * 20 + a
            ca[:20, q] = h[a]
            ci[:20, q] = h[ii]
            for k in range(3):
                folds[0, q, 32 * k + a] = 1
                folds[1, q, 32 * k + ii] = 1
        order = h[ii].reshape(2, 10).T.reshape(-1)
        for k in range(3):
            wide[0, ii, 80 * k : 80 * k + 80] = np.repeat(order, 4)
        for y in range(20):
            wide[1, ii, y * ZPAD : y * ZPAD + 20] = h[ii, y]
            wide[2, ii, y * ZPAD : y * ZPAD + 20] = h[ii]
    high = np.asarray(np.asarray(wide, np.float32).astype(jnp.bfloat16), np.float32)
    c["wide"] = np.concatenate([high, high, wide - high, np.zeros((3, 32, LANES))], axis=1)
    c["ca"], c["ci"], c["folds"] = ca, ci, folds
    po = np.zeros((160, 160))
    for xx in range(20):
        for r in range(8):
            po[(r // 2) * 40 + (r % 2) * 20 + xx, (r // 4) * 80 + xx * 4 + r % 4] = 1
    c["po"] = po
    return c


def _onehot(t):
    return jnp.asarray(t, BF16)


def _pair(t):
    t = np.asarray(t, np.float32)
    hi = t.astype(jnp.bfloat16)
    lo = (t - hi.astype(np.float32)).astype(jnp.bfloat16)
    return jnp.asarray(np.stack([hi, lo]))


def dot(a, b):
    return jnp.dot(a, b, preferred_element_type=F32)


def dot_nt(a, b):
    return lax.dot_general(a, b, (((1,), (1,)), ((), ())), preferred_element_type=F32)


def split2(v):
    hi = v.astype(BF16)
    return hi, (v - hi.astype(F32)).astype(BF16)


def split3(v):
    hi = v.astype(BF16)
    rest = v - hi.astype(F32)
    mid = rest.astype(BF16)
    return hi, mid, (rest - mid.astype(F32)).astype(BF16)


def dot3(a, b):
    ah, al = a
    bh, bl = b
    return dot(ah, bh) + (dot(al, bh) + dot(ah, bl))


def iota(shape, dim):
    return lax.broadcasted_iota(jnp.int32, shape, dim)


def placed(lanes):
    return (iota((LANES, LANES), 0) == lanes).astype(F32).astype(BF16)


def pack_kernel(leaf, td, ts, ct, pp, lanes, ra, hx, hy, wmsg, cmsg, rows):
    perm = placed(lanes[0:1, :])
    rows[...] = jnp.zeros_like(rows)
    for a in range(ORDER):
        rows[16 * a : 16 * a + 16, :100] = leaf[:, 100 * a : 100 * a + 100]
    w = jnp.zeros((40, LANES), F32)
    for part in split3(rows[...]):
        pieces = [dot(ra[o], part) for o in range(4)]
        w = w + dot(jnp.concatenate(pieces, axis=1).astype(BF16), perm)
    first = dot3((hx[0], hx[1]), split2(w))
    corner = dot3(split2(first), (hy[0], hy[1]))
    lane = iota((40, LANES), 1)
    row = iota((40, LANES), 0)
    for n in range(NODES1):
        mine = (row // EDGE) == n
        for e in range(DISP):
            w = jnp.where(mine & (lane == 480 + e), td[n, e].astype(F32), w)
            w = jnp.where(mine & (lane == 488 + e), ts[n, e].astype(F32), w)
    wmsg[...] = w
    z = lax.axis_index("gz")
    lane2 = iota((24, 128), 1)
    row2 = iota((24, 128), 0)
    for n in range(NODES1):
        q = pp[0, z * NODES1 + n]
        corner = jnp.where((row2 == n) & (lane2 == 108), (q % 8).astype(F32), corner)
        for e in range(DISP):
            here = (row2 == n) & (lane2 == 100 + e)
            corner = jnp.where(here, ct[q // 8, e].astype(F32), corner)
    for k in range(32):
        cmsg[k] = corner


def prep_kernel(ob, ranks, ci, ca, folds, wide, a0, l1, l2, q0, q1, q2):
    level = pl.program_id(0)
    for e in range(DISP):
        for t in range(TERMS):
            k = e * TERMS + t
            keep = (t < ranks[level, e]).astype(F32)
            q0[24 * k : 24 * k + 24, :] = ob[0, e, 0, t : t + 1, :] * keep * ci[...]
            q1[24 * k : 24 * k + 24, :] = ob[0, e, 1, t : t + 1, :] * ca[...]
            q2[24 * k : 24 * k + 24, :] = ob[0, e, 2, t : t + 1, :] * ca[...]

    def folded(q, fold, d):
        hi, lo = split2(q[...])
        both = dot(hi, fold) + dot(lo, fold)
        lane = iota(both.shape, 1) // 32
        rest = both - both.astype(BF16).astype(F32)
        return dot(jnp.where(lane == 1, rest, both).astype(BF16), wide[d])

    a0[0] = folded(q0, folds[0], 0)[:, :256].reshape(PAIRS, ZPAD, 256)
    l1[0] = folded(q1, folds[1], 1).reshape(PAIRS, ZPAD, LANES)
    l2[0] = folded(q2, folds[1], 2).reshape(PAIRS, ZPAD, LANES)


def fetch(level, mats, a0, l1, l2, sems):
    targets = (a0, l1, l2)
    return [pltpu.make_async_copy(m.at[level], t, sems.at[i]) for i, (m, t) in enumerate(zip(mats, targets))]


def images(ranks, level, groups, scat, a0, l1, l2, acc, kh, kl, zs, bd, order):
    count = sum(ranks[level, e] for e in range(DISP))
    base = 0
    for e in range(DISP):
        rank = ranks[level, e]
        for t in range(TERMS):
            dropped = count + (TERMS * e - base) + (t - rank)
            order[jnp.where(t < rank, base + t, dropped)] = TERMS * e + t
        base = base + rank
    rows = 80 * groups
    acc[...] = jnp.zeros_like(acc)
    for slot in range(2):
        kh[slot, 480:, :] = jnp.zeros((32, LANES), BF16)
        kl[slot, 480:, :] = jnp.zeros((32, LANES), BF16)
    lane = iota((8, 256), 1)
    row = iota((8, 256), 0)
    same = jnp.where((lane % 4 == row % 4) & (lane < 240), 1.0, 0.0)

    def prepare(k, slot):
        at = order[k]
        for i in range(0, EDGE, 2):
            value = jnp.where(row < 4, a0[at, i : i + 1, :], a0[at, i + 1 : i + 2, :]) * same
            rest = value - value.astype(BF16).astype(F32)
            bd[slot, 4 * i : 4 * i + 8, :] = jnp.where(lane < 160, value, rest)
        left = bd[slot].astype(BF16)
        for g in range(groups):
            hi, lo = split2(dot(left, scat[at // TERMS, g]))
            zs[slot, 80 * g : 80 * g + 80, :] = hi
            zs[slot, rows + 80 * g : rows + 80 * g + 80, :] = lo
        third = l2[at]
        for y in range(0, EDGE, 2):
            one = l1[at, y : y + 1, :] * third
            two = l1[at, y + 1 : y + 2, :] * third
            hi, lo = split2(jnp.concatenate([one, two], axis=0))
            kh[slot, ZPAD * y : ZPAD * y + 48, :] = hi
            kl[slot, ZPAD * y : ZPAD * y + 48, :] = lo

    def term(slot):
        both = dot(zs[slot], kh[slot])
        rest = dot(zs[slot, :rows, :], kl[slot])
        acc[...] = acc[...] + ((both[:rows] + rest) + both[rows:])

    prepare(0, 0)

    def step(j, carry):
        prepare(2 * j + 1, 1)
        term(0)
        prepare(jnp.minimum(2 * j + 2, PAIRS - 1), 0)
        term(1)
        return carry

    lax.fori_loop(0, (count + 1) // 2, step, 0)


def sources(hi, lo):
    return jnp.concatenate([hi, lo, hi, jnp.zeros((16, LANES), BF16)], axis=0)


def coarse_kernel(
    corners, pp, ranks, m0, m1, m2, lanes, out, scat, acc, kh, kl, zs, bd, order, a0, l1, l2, sems, gs, sw, perm
):
    copies = fetch(0, (m0, m1, m2), a0, l1, l2, sems)
    for copy in copies:
        copy.start()
    perm[...] = placed(lanes[0:1, :])
    parts = []
    for a in range(ORDER):
        pair = [corners[pl.ds(2 * a + n, 32, stride=24), :] for n in range(NODES1)]
        parts.append(jnp.concatenate(pair, axis=0))
    value = jnp.concatenate(parts, axis=1)
    sel = (iota((16, 128), 1) == iota((16, 128), 0) + 100).astype(F32).astype(BF16)
    index = value[:, 0:128].astype(BF16)
    info = dot_nt(sel, jnp.concatenate([index, index], axis=0))
    col = lax.axis_index("gx") * lax.axis_size("gy") + lax.axis_index("gy")
    r4 = iota((8, 128), 0) % 4
    ox = iota((8, 128), 0) // 4
    want = jnp.where(r4 < C0, (col * C0 + r4), -1).astype(F32)
    octant = info[8:9, :]
    blocks = []
    for oyz in range(4):
        there = octant == (4 * ox + oyz).astype(F32)
        for d in range(DISP):
            blocks.append(jnp.where((info[d : d + 1, :] == want) & there, 1.0, 0.0))
    pick = jnp.concatenate(blocks, axis=0).astype(BF16)
    summed = dot(pick, jnp.concatenate(split2(value), axis=0))
    gs[...] = summed.reshape(4 * DISP, 8, 1280)

    def place(e, carry):
        for oyz in range(4):
            for a in range(ORDER):
                sw[8 * a : 8 * a + 8, 128 * oyz : 128 * oyz + 128] = gs[
                    oyz * DISP + e, :, 128 * a : 128 * a + 128
                ]
        moved = dot(jnp.concatenate(split2(sw[...]), axis=0), perm[...]).astype(BF16)
        scat[e, 0] = sources(moved[:80], moved[80:])
        return carry

    lax.fori_loop(0, DISP, place, 0)
    for copy in copies:
        copy.wait()
    images(ranks, 0, 1, scat, a0, l1, l2, acc, kh, kl, zs, bd, order)
    back = placed(lanes[1:2, :])
    at = iota((ZPAD, 320), 1)
    code = ((at % 4) * 4 + at // 80) * EDGE + (at % 80) // 4
    row = iota((ZPAD, 320), 0)
    a = row % 12
    blocks = []
    for z in range(8):
        qs = [pp[0, NODES1 * z + n] for n in range(NODES1)]
        bases = [((q // 8) * 4 + q % 4) * EDGE + ((q % 8) // 4) * ORDER for q in qs]
        base = jnp.where(row < 12, bases[0], bases[1])
        blocks.append(jnp.where((a < ORDER) & (code == base + a), 1.0, 0.0))
    pick = jnp.concatenate(blocks, axis=0).astype(BF16)
    picked = jnp.zeros((192, 128), F32)
    moved = dot(jnp.concatenate(split3(acc[...]), axis=0), back).astype(BF16)
    for k in range(3):
        part = moved[80 * k : 80 * k + 80, :]
        stacked = jnp.concatenate([part[:, 128 * o : 128 * o + 128] for o in range(4)], axis=0)
        picked = picked + dot(pick, stacked)
    for z in range(8):
        out[z] = picked[ZPAD * z : ZPAD * z + ZPAD, :]


def middle_kernel(*refs):
    walls, refs = refs[:8], refs[8:]
    ranks, m0, m1, m2, po, out0, out1, out2, out3, scat, acc, kh, kl, zs, bd, order, a0, l1, l2, sems, info, wcat = refs
    copies = fetch(1, (m0, m1, m2), a0, l1, l2, sems)
    for copy in copies:
        copy.start()
    sel = (iota((16, 128), 1) == iota((16, 128), 0) + 96).astype(F32).astype(BF16)
    wall = jnp.concatenate([w[...] for w in walls], axis=0)
    index = wall[:, 384:512].astype(BF16)
    raw = dot_nt(sel, jnp.concatenate([index, index], axis=0))
    device = raw[0:8, :]
    gy = jnp.floor(device * 0.125)
    gz = device - gy * 8.0
    z = lax.axis_index("gz").astype(F32)
    info[...] = jnp.where(gz == z, gy * 2.0 + raw[8:16, :], -1.0).reshape(8, 1, 640)
    hi, lo = split2(wall)
    wcat[0:320, :] = hi
    wcat[320:640, :] = lo
    lane = iota((160, 640), 1) % EDGE
    row = iota((160, 640), 0)
    slot = ((row // 80) * 4 + row % 4).astype(F32)
    fits = lane == ((row % 8) // 4) * ORDER + (row % 80) // 8

    def place(e, carry):
        pick = jnp.where(fits & (info[e] == slot), 1.0, 0.0).astype(BF16)
        high, low = split2(dot(pick, wcat[...]))
        for g in range(2):
            scat[e, g] = sources(high[80 * g : 80 * g + 80], low[80 * g : 80 * g + 80])
        return carry

    lax.fori_loop(0, DISP, place, 0)
    for copy in copies:
        copy.wait()
    images(ranks, 1, 2, scat, a0, l1, l2, acc, kh, kl, zs, bd, order)
    moved = jnp.zeros((160, LANES), F32)
    for part in split3(acc[...]):
        moved = moved + dot(po[...], part)
    acc[...] = moved
    own = lax.axis_index("gy")
    for k, out in enumerate((out0, out1, out2, out3)):
        out[...] = acc[pl.ds(pl.multiple_of((own + k) % 4 * 40, 8), 40), :]


def final_kernel(mid0, mid1, mid2, mid3, coarse, lanes, ht, hyt, rt, out):
    back = placed(lanes[1:2, :])
    total = (mid0[...] + mid1[...]) + (mid2[...] + mid3[...])
    corner = coarse[0]
    for z in range(1, 8):
        corner = corner + coarse[z]
    up = dot3((ht[0], ht[1]), split2(corner))
    total = total + dot3(split2(up), (hyt[0], hyt[1]))
    rows = jnp.zeros((160, 128), F32)
    for part in split3(total):
        moved = dot(part, back).astype(BF16)
        stacked = jnp.concatenate([moved[:, 128 * o : 128 * o + 128] for o in range(4)], axis=0)
        rows = rows + dot(rt[...], stacked)
    for a in range(ORDER):
        out[:, 100 * a : 100 * a + 100] = rows[16 * a : 16 * a + 16, :100]


AN = pl.BlockSpec(memory_space=pl.ANY)
VM = pl.BlockSpec(memory_space=pltpu.MemorySpace.VMEM)
SM = pl.BlockSpec(memory_space=pltpu.MemorySpace.SMEM)
COST = pl.CostEstimate(flops=8_000_000_000, transcendentals=0, bytes_accessed=4_000_000)


def local(value):
    return pltpu.with_memory_space_constraint(value, pltpu.VMEM)


def sds(*shape):
    return jax.ShapeDtypeStruct(shape, F32)


def _params():
    return pltpu.CompilerParams(vmem_limit_bytes=56 * 1024 * 1024)


def level_scratch(groups):
    rows = 80 * groups
    return [
        pltpu.VMEM((DISP, groups, 256, LANES), BF16),
        pltpu.VMEM((rows, LANES), F32),
        pltpu.VMEM((2, LANES, LANES), BF16),
        pltpu.VMEM((2, LANES, LANES), BF16),
        pltpu.VMEM((2, 2 * rows, LANES), BF16),
        pltpu.VMEM((2, 80, 256), F32),
        pltpu.SMEM((32,), jnp.int32),
        *[pltpu.VMEM((PAIRS, ZPAD, n), F32) for n in (256, LANES, LANES)],
        pltpu.SemaphoreType.DMA((3,)),
    ]


def const(shape):
    return pl.BlockSpec(shape, lambda *_: (0,) * len(shape))


def shifted(value, axis, by):
    size = lax.axis_size(axis)
    return lax.ppermute(value, axis, [(i, (i + by) % size) for i in range(size)])


def swap(value, axis):
    return lax.all_to_all(value, axis, split_axis=0, concat_axis=0, tiled=True)


def on_device(leaf, ob, ranks, td, ts, ct, pp):
    c = _tables()
    lanes = jnp.asarray(c["lanes"], jnp.int32)
    wmsg, cmsg = pl.pallas_call(
        pack_kernel,
        out_shape=(sds(40, LANES), sds(32, 24, 128)),
        in_specs=[VM, SM, SM, SM, SM, VM, VM, VM, VM],
        out_specs=(VM, VM),
        scratch_shapes=[pltpu.VMEM((160, 128), F32)],
        compiler_params=_params(),
        name="pack",
    )(
        leaf,
        td.reshape(NODES1, DISP),
        ts,
        ct,
        pp,
        lanes,
        _onehot(c["ra"]),
        _pair(c["hx"]),
        _pair(c["hy"]),
    )
    corners = swap(cmsg, ("gx", "gy")).reshape(768, 128)
    rows = DISP * TERMS * 24
    mats = pl.pallas_call(
        prep_kernel,
        grid=(2,),
        out_shape=tuple(sds(2, PAIRS, ZPAD, n) for n in (256, LANES, LANES)),
        in_specs=[
            pl.BlockSpec((1, DISP, 3, TERMS, 400), lambda l: (l, 0, 0, 0, 0)),
            SM,
            const((24, 400)),
            const((24, 400)),
            const((2, 400, 128)),
            const((3, 128, LANES)),
        ],
        out_specs=tuple(
            pl.BlockSpec((1, PAIRS, ZPAD, n), lambda l: (l, 0, 0, 0)) for n in (256, LANES, LANES)
        ),
        scratch_shapes=[pltpu.VMEM((rows, 400), F32)] * 3,
        compiler_params=_params(),
        cost_estimate=COST,
        name="prep",
    )(ob.transpose(0, 1, 3, 2, 4), ranks, jnp.asarray(c["ci"]), jnp.asarray(c["ca"]), _onehot(c["folds"]), _onehot(c["wide"]))
    wall = [wmsg] + [local(shifted(wmsg, "gz", k)) for k in range(1, 8)]

    coarse = pl.pallas_call(
        coarse_kernel,
        out_shape=sds(8, 24, 128),
        in_specs=[VM, SM, SM, AN, AN, AN, VM],
        out_specs=VM,
        scratch_shapes=[
            *level_scratch(1),
            pltpu.VMEM((4 * DISP, 8, 1280), F32),
            pltpu.VMEM((80, LANES), F32),
            pltpu.VMEM((LANES, LANES), BF16),
        ],
        compiler_params=_params(),
        cost_estimate=COST,
        name="coarse",
    )(local(corners), pp, ranks, *mats, lanes)
    middle = pl.pallas_call(
        middle_kernel,
        out_shape=(sds(40, LANES),) * 4,
        in_specs=[*[VM] * 8, SM, AN, AN, AN, VM],
        out_specs=(VM,) * 4,
        scratch_shapes=[
            *level_scratch(2),
            pltpu.VMEM((8, 1, 640), F32),
            pltpu.VMEM((640, LANES), BF16),
        ],
        compiler_params=_params(),
        cost_estimate=COST,
        name="middle",
    )(*wall, ranks, *mats, _onehot(c["po"]))
    coarse = swap(coarse, "gz")
    middle = [middle[0]] + [local(shifted(m, "gy", k + 1)) for k, m in enumerate(middle[1:])]
    return pl.pallas_call(
        final_kernel,
        out_shape=sds(16, 1000),
        in_specs=[VM] * 9,
        out_specs=VM,
        compiler_params=_params(),
        name="final",
    )(*middle, local(coarse), lanes, _pair(c["ht"]), _pair(c["hyt"]), _onehot(c["rt"]))


def solution(mesh):
    in_specs = (
        P(("gx", "gy", "gz"), None),
        P(),
        P(),
        P(("gx", "gy", "gz"), None, None),
        P(("gx", "gy", "gz"), None),
        P(("gx", "gy"), None),
        P(("gx", "gy"), None),
    )
    out_specs = P(("gx", "gy", "gz"), None)
    return jax.shard_map(
        on_device, mesh=mesh, in_specs=in_specs, out_specs=out_specs, check_vma=False
    )
```

```python
import jax
import jax.numpy as jnp
import numpy as np
from jax import lax
from jax.experimental import pallas as pl
from jax.experimental.pallas import tpu as pltpu
from jax.sharding import PartitionSpec as P

ORDER = 10
EDGE = 20
ZPAD = 24
LANES = 512
DISP = 7
TERMS = 4
SLOTS = 8
C0 = 3
NODES1 = 2
PAIRS = DISP * TERMS
F32 = jnp.float32
BF16 = jnp.bfloat16


def _tables():
    n = EDGE
    i = np.arange(n)[:, None]
    x = np.arange(n)[None, :]
    h = np.sqrt(2.0 / n) * np.cos(np.pi * (x + 0.5) * i / n)
    h[0] *= np.sqrt(0.5)
    c = {}
    lanes = np.full((8, LANES), -1)
    for y in range(EDGE):
        for z in range(EDGE):
            at = (2 * (y // 10) + z // 10) * 128 + (y % 10) * 10 + z % 10
            lanes[0, y * ZPAD + z] = at
            lanes[1, at] = y * ZPAD + z
    c["lanes"] = lanes
    ra = np.zeros((4, 40, 160))
    rt = np.zeros((160, 160))
    for nn in range(2):
        for ox in range(2):
            for oyz in range(4):
                for a in range(10):
                    row = nn * 20 + ox * 10 + a
                    leaf = 8 * nn + 4 * ox + oyz
                    ra[oyz, row, a * 16 + leaf] = 1
                    rt[a * 16 + leaf, oyz * 40 + row] = 1
    c["ra"] = ra
    c["rt"] = rt
    hx = np.zeros((24, 40))
    ht = np.zeros((40, 24))
    for nn in range(2):
        for ii in range(10):
            for xx in range(20):
                hx[ii * 2 + nn, nn * 20 + xx] = h[ii, xx]
                ht[nn * 20 + xx, nn * 12 + ii] = h[ii, xx]
    c["hx"] = hx
    c["ht"] = ht
    hy = np.zeros((LANES, 128))
    for y in range(20):
        for z in range(20):
            hy[y * ZPAD + z, :100] = np.outer(h[:10, y], h[:10, z]).reshape(-1)
    c["hy"] = hy
    c["hyt"] = hy.T.copy()
    ca = np.zeros((24, 400))
    ci = np.zeros((24, 400))
    folds = np.zeros((2, 400, 128))
    wide = np.zeros((3, 32, LANES))
    for ii in range(20):
        for a in range(20):
            q = ii * 20 + a
            ca[:20, q] = h[a]
            ci[:20, q] = h[ii]
            for k in range(3):
                folds[0, q, 32 * k + a] = 1
                folds[1, q, 32 * k + ii] = 1
        order = h[ii].reshape(2, 10).T.reshape(-1)
        for k in range(3):
            wide[0, ii, 80 * k : 80 * k + 80] = np.repeat(order, 4)
        for y in range(20):
            wide[1, ii, y * ZPAD : y * ZPAD + 20] = h[ii, y]
            wide[2, ii, y * ZPAD : y * ZPAD + 20] = h[ii]
    high = np.asarray(np.asarray(wide, np.float32).astype(jnp.bfloat16), np.float32)
    c["wide"] = np.concatenate([high, high, wide - high, np.zeros((3, 32, LANES))], axis=1)
    c["ca"], c["ci"], c["folds"] = ca, ci, folds
    po = np.zeros((160, 160))
    for xx in range(20):
        for r in range(8):
            po[(r // 2) * 40 + (r % 2) * 20 + xx, (r // 4) * 80 + xx * 4 + r % 4] = 1
    c["po"] = po
    return c


def _onehot(t):
    return jnp.asarray(t, BF16)


def _pair(t):
    t = np.asarray(t, np.float32)
    hi = t.astype(jnp.bfloat16)
    lo = (t - hi.astype(np.float32)).astype(jnp.bfloat16)
    return jnp.asarray(np.stack([hi, lo]))


def dot(a, b):
    return jnp.dot(a, b, preferred_element_type=F32)


def dot_nt(a, b):
    return lax.dot_general(a, b, (((1,), (1,)), ((), ())), preferred_element_type=F32)


def split2(v):
    hi = v.astype(BF16)
    return hi, (v - hi.astype(F32)).astype(BF16)


def split3(v):
    hi = v.astype(BF16)
    rest = v - hi.astype(F32)
    mid = rest.astype(BF16)
    return hi, mid, (rest - mid.astype(F32)).astype(BF16)


def dot3(a, b):
    ah, al = a
    bh, bl = b
    return dot(ah, bh) + (dot(al, bh) + dot(ah, bl))


def iota(shape, dim):
    return lax.broadcasted_iota(jnp.int32, shape, dim)


def placed(lanes):
    return (iota((LANES, LANES), 0) == lanes).astype(F32).astype(BF16)


def pack_kernel(leaf, td, ts, ct, pp, lanes, ra, hx, hy, wmsg, cmsg, rows):
    perm = placed(lanes[0:1, :])
    rows[...] = jnp.zeros_like(rows)
    for a in range(ORDER):
        rows[16 * a : 16 * a + 16, :100] = leaf[:, 100 * a : 100 * a + 100]
    w = jnp.zeros((40, LANES), F32)
    for part in split3(rows[...]):
        pieces = [dot(ra[o], part) for o in range(4)]
        w = w + dot(jnp.concatenate(pieces, axis=1).astype(BF16), perm)
    first = dot3((hx[0], hx[1]), split2(w))
    corner = dot3(split2(first), (hy[0], hy[1]))
    lane = iota((40, LANES), 1)
    row = iota((40, LANES), 0)
    for n in range(NODES1):
        mine = (row // EDGE) == n
        for e in range(DISP):
            w = jnp.where(mine & (lane == 480 + e), td[n, e].astype(F32), w)
            w = jnp.where(mine & (lane == 488 + e), ts[n, e].astype(F32), w)
    wmsg[...] = w
    z = lax.axis_index("gz")
    lane2 = iota((24, 128), 1)
    row2 = iota((24, 128), 0)
    for n in range(NODES1):
        q = pp[0, z * NODES1 + n]
        corner = jnp.where((row2 == n) & (lane2 == 108), (q % 8).astype(F32), corner)
        for e in range(DISP):
            here = (row2 == n) & (lane2 == 100 + e)
            corner = jnp.where(here, ct[q // 8, e].astype(F32), corner)
    for k in range(32):
        cmsg[k] = corner


def prep_kernel(ob, ranks, ci, ca, folds, wide, a0, l1, l2, q0, q1, q2):
    level = pl.program_id(0)
    for e in range(DISP):
        for t in range(TERMS):
            k = e * TERMS + t
            keep = (t < ranks[level, e]).astype(F32)
            q0[24 * k : 24 * k + 24, :] = ob[0, e, 0, t : t + 1, :] * keep * ci[...]
            q1[24 * k : 24 * k + 24, :] = ob[0, e, 1, t : t + 1, :] * ca[...]
            q2[24 * k : 24 * k + 24, :] = ob[0, e, 2, t : t + 1, :] * ca[...]

    def folded(q, fold, d):
        hi, lo = split2(q[...])
        both = dot(hi, fold) + dot(lo, fold)
        lane = iota(both.shape, 1) // 32
        rest = both - both.astype(BF16).astype(F32)
        return dot(jnp.where(lane == 1, rest, both).astype(BF16), wide[d])

    a0[0] = folded(q0, folds[0], 0)[:, :256].reshape(PAIRS, ZPAD, 256)
    l1[0] = folded(q1, folds[1], 1).reshape(PAIRS, ZPAD, LANES)
    l2[0] = folded(q2, folds[1], 2).reshape(PAIRS, ZPAD, LANES)


def fetch(level, mats, a0, l1, l2, sems):
    targets = (a0, l1, l2)
    return [pltpu.make_async_copy(m.at[level], t, sems.at[i]) for i, (m, t) in enumerate(zip(mats, targets))]


def images(ranks, level, groups, scat, a0, l1, l2, acc, kh, kl, zs, bd, order):
    count = sum(ranks[level, e] for e in range(DISP))
    base = 0
    for e in range(DISP):
        rank = ranks[level, e]
        for t in range(TERMS):
            dropped = count + (TERMS * e - base) + (t - rank)
            order[jnp.where(t < rank, base + t, dropped)] = TERMS * e + t
        base = base + rank
    rows = 80 * groups
    acc[...] = jnp.zeros_like(acc)
    for slot in range(2):
        kh[slot, 480:, :] = jnp.zeros((32, LANES), BF16)
        kl[slot, 480:, :] = jnp.zeros((32, LANES), BF16)
    lane = iota((8, 256), 1)
    row = iota((8, 256), 0)
    same = jnp.where((lane % 4 == row % 4) & (lane < 240), 1.0, 0.0)

    def prepare(k, slot):
        at = order[k]
        for i in range(0, EDGE, 2):
            value = jnp.where(row < 4, a0[at, i : i + 1, :], a0[at, i + 1 : i + 2, :]) * same
            rest = value - value.astype(BF16).astype(F32)
            bd[slot, 4 * i : 4 * i + 8, :] = jnp.where(lane < 160, value, rest)
        left = bd[slot].astype(BF16)
        for g in range(groups):
            hi, lo = split2(dot(left, scat[at // TERMS, g]))
            zs[slot, 80 * g : 80 * g + 80, :] = hi
            zs[slot, rows + 80 * g : rows + 80 * g + 80, :] = lo
        third = l2[at]
        for y in range(0, EDGE, 2):
            one = l1[at, y : y + 1, :] * third
            two = l1[at, y + 1 : y + 2, :] * third
            hi, lo = split2(jnp.concatenate([one, two], axis=0))
            kh[slot, ZPAD * y : ZPAD * y + 48, :] = hi
            kl[slot, ZPAD * y : ZPAD * y + 48, :] = lo

    def term(slot):
        both = dot(zs[slot], kh[slot])
        rest = dot(zs[slot, :rows, :], kl[slot])
        acc[...] = acc[...] + ((both[:rows] + rest) + both[rows:])

    prepare(0, 0)

    def step(j, carry):
        prepare(2 * j + 1, 1)
        term(0)
        prepare(jnp.minimum(2 * j + 2, PAIRS - 1), 0)
        term(1)
        return carry

    lax.fori_loop(0, (count + 1) // 2, step, 0)


def sources(hi, lo):
    return jnp.concatenate([hi, lo, hi, jnp.zeros((16, LANES), BF16)], axis=0)


def coarse_kernel(
    corners, pp, ranks, m0, m1, m2, lanes, out, scat, acc, kh, kl, zs, bd, order, a0, l1, l2, sems, gs, sw, perm
):
    copies = fetch(0, (m0, m1, m2), a0, l1, l2, sems)
    for copy in copies:
        copy.start()
    perm[...] = placed(lanes[0:1, :])
    parts = []
    for a in range(ORDER):
        pair = [corners[pl.ds(2 * a + n, 32, stride=24), :] for n in range(NODES1)]
        parts.append(jnp.concatenate(pair, axis=0))
    value = jnp.concatenate(parts, axis=1)
    sel = (iota((16, 128), 1) == iota((16, 128), 0) + 100).astype(F32).astype(BF16)
    index = value[:, 0:128].astype(BF16)
    info = dot_nt(sel, jnp.concatenate([index, index], axis=0))
    col = lax.axis_index("gx") * lax.axis_size("gy") + lax.axis_index("gy")
    r4 = iota((8, 128), 0) % 4
    ox = iota((8, 128), 0) // 4
    want = jnp.where(r4 < C0, (col * C0 + r4), -1).astype(F32)
    octant = info[8:9, :]
    blocks = []
    for oyz in range(4):
        there = octant == (4 * ox + oyz).astype(F32)
        for d in range(DISP):
            blocks.append(jnp.where((info[d : d + 1, :] == want) & there, 1.0, 0.0))
    pick = jnp.concatenate(blocks, axis=0).astype(BF16)
    summed = dot(pick, jnp.concatenate(split2(value), axis=0))
    gs[...] = summed.reshape(4 * DISP, 8, 1280)

    def place(e, carry):
        for oyz in range(4):
            for a in range(ORDER):
                sw[8 * a : 8 * a + 8, 128 * oyz : 128 * oyz + 128] = gs[
                    oyz * DISP + e, :, 128 * a : 128 * a + 128
                ]
        moved = dot(jnp.concatenate(split2(sw[...]), axis=0), perm[...]).astype(BF16)
        scat[e, 0] = sources(moved[:80], moved[80:])
        return carry

    lax.fori_loop(0, DISP, place, 0)
    for copy in copies:
        copy.wait()
    images(ranks, 0, 1, scat, a0, l1, l2, acc, kh, kl, zs, bd, order)
    back = placed(lanes[1:2, :])
    at = iota((ZPAD, 320), 1)
    code = ((at % 4) * 4 + at // 80) * EDGE + (at % 80) // 4
    row = iota((ZPAD, 320), 0)
    a = row % 12
    blocks = []
    for z in range(8):
        qs = [pp[0, NODES1 * z + n] for n in range(NODES1)]
        bases = [((q // 8) * 4 + q % 4) * EDGE + ((q % 8) // 4) * ORDER for q in qs]
        base = jnp.where(row < 12, bases[0], bases[1])
        blocks.append(jnp.where((a < ORDER) & (code == base + a), 1.0, 0.0))
    pick = jnp.concatenate(blocks, axis=0).astype(BF16)
    picked = jnp.zeros((192, 128), F32)
    moved = dot(jnp.concatenate(split3(acc[...]), axis=0), back).astype(BF16)
    for k in range(3):
        part = moved[80 * k : 80 * k + 80, :]
        stacked = jnp.concatenate([part[:, 128 * o : 128 * o + 128] for o in range(4)], axis=0)
        picked = picked + dot(pick, stacked)
    for z in range(8):
        out[z] = picked[ZPAD * z : ZPAD * z + ZPAD, :]


def middle_kernel(*refs):
    walls, refs = refs[:2], refs[2:]
    ranks, m0, m1, m2, po, out0, out1, out2, out3, scat, acc, kh, kl, zs, bd, order, a0, l1, l2, sems, info, wcat = refs
    copies = fetch(1, (m0, m1, m2), a0, l1, l2, sems)
    for copy in copies:
        copy.start()
    sel = (iota((16, 128), 1) == iota((16, 128), 0) + 96).astype(F32).astype(BF16)
    wall = jnp.concatenate([w[...] for w in walls], axis=0)
    index = wall[:, 384:512].astype(BF16)
    raw = dot_nt(sel, jnp.concatenate([index, index], axis=0))
    device = raw[0:8, :]
    gy = jnp.floor(device * 0.125)
    gz = device - gy * 8.0
    z = lax.axis_index("gz").astype(F32)
    info[...] = jnp.where(gz == z, gy * 2.0 + raw[8:16, :], -1.0).reshape(8, 1, 640)
    hi, lo = split2(wall)
    wcat[0:320, :] = hi
    wcat[320:640, :] = lo
    lane = iota((160, 640), 1) % EDGE
    row = iota((160, 640), 0)
    slot = ((row // 80) * 4 + row % 4).astype(F32)
    fits = lane == ((row % 8) // 4) * ORDER + (row % 80) // 8

    def place(e, carry):
        pick = jnp.where(fits & (info[e] == slot), 1.0, 0.0).astype(BF16)
        high, low = split2(dot(pick, wcat[...]))
        for g in range(2):
            scat[e, g] = sources(high[80 * g : 80 * g + 80], low[80 * g : 80 * g + 80])
        return carry

    lax.fori_loop(0, DISP, place, 0)
    for copy in copies:
        copy.wait()
    images(ranks, 1, 2, scat, a0, l1, l2, acc, kh, kl, zs, bd, order)
    moved = jnp.zeros((160, LANES), F32)
    for part in split3(acc[...]):
        moved = moved + dot(po[...], part)
    acc[...] = moved
    own = lax.axis_index("gy")
    for k, out in enumerate((out0, out1, out2, out3)):
        out[...] = acc[pl.ds(pl.multiple_of((own + k) % 4 * 40, 8), 40), :]


def final_kernel(mid0, mid1, mid2, mid3, coarse, lanes, ht, hyt, rt, out):
    back = placed(lanes[1:2, :])
    total = (mid0[...] + mid1[...]) + (mid2[...] + mid3[...])
    corner = coarse[0]
    for z in range(1, 8):
        corner = corner + coarse[z]
    up = dot3((ht[0], ht[1]), split2(corner))
    total = total + dot3(split2(up), (hyt[0], hyt[1]))
    rows = jnp.zeros((160, 128), F32)
    for part in split3(total):
        moved = dot(part, back).astype(BF16)
        stacked = jnp.concatenate([moved[:, 128 * o : 128 * o + 128] for o in range(4)], axis=0)
        rows = rows + dot(rt[...], stacked)
    for a in range(ORDER):
        out[:, 100 * a : 100 * a + 100] = rows[16 * a : 16 * a + 16, :100]


AN = pl.BlockSpec(memory_space=pl.ANY)
VM = pl.BlockSpec(memory_space=pltpu.MemorySpace.VMEM)
SM = pl.BlockSpec(memory_space=pltpu.MemorySpace.SMEM)
COST = pl.CostEstimate(flops=8_000_000_000, transcendentals=0, bytes_accessed=4_000_000)


def local(value):
    return pltpu.with_memory_space_constraint(value, pltpu.VMEM)


def sds(*shape):
    return jax.ShapeDtypeStruct(shape, F32)


def _params():
    return pltpu.CompilerParams(vmem_limit_bytes=56 * 1024 * 1024)


def level_scratch(groups):
    rows = 80 * groups
    return [
        pltpu.VMEM((DISP, groups, 256, LANES), BF16),
        pltpu.VMEM((rows, LANES), F32),
        pltpu.VMEM((2, LANES, LANES), BF16),
        pltpu.VMEM((2, LANES, LANES), BF16),
        pltpu.VMEM((2, 2 * rows, LANES), BF16),
        pltpu.VMEM((2, 80, 256), F32),
        pltpu.SMEM((32,), jnp.int32),
        *[pltpu.VMEM((PAIRS, ZPAD, n), F32) for n in (256, LANES, LANES)],
        pltpu.SemaphoreType.DMA((3,)),
    ]


def const(shape):
    return pl.BlockSpec(shape, lambda *_: (0,) * len(shape))


def shifted(value, axis, by):
    size = lax.axis_size(axis)
    return lax.ppermute(value, axis, [(i, (i + by) % size) for i in range(size)])


def traded(value, axis, bit):
    return lax.ppermute(value, axis, [(i, i ^ bit) for i in range(lax.axis_size(axis))])


def swap(value, axis):
    return lax.all_to_all(value, axis, split_axis=0, concat_axis=0, tiled=True)


def on_device(leaf, ob, ranks, td, ts, ct, pp):
    c = _tables()
    lanes = jnp.asarray(c["lanes"], jnp.int32)
    wmsg, cmsg = pl.pallas_call(
        pack_kernel,
        out_shape=(sds(40, LANES), sds(32, 24, 128)),
        in_specs=[VM, SM, SM, SM, SM, VM, VM, VM, VM],
        out_specs=(VM, VM),
        scratch_shapes=[pltpu.VMEM((160, 128), F32)],
        compiler_params=_params(),
        name="pack",
    )(
        leaf,
        td.reshape(NODES1, DISP),
        ts,
        ct,
        pp,
        lanes,
        _onehot(c["ra"]),
        _pair(c["hx"]),
        _pair(c["hy"]),
    )
    wall = jnp.concatenate([wmsg, traded(wmsg, "gz", 1)], axis=0)
    corners = swap(cmsg, ("gx", "gy")).reshape(768, 128)
    rows = DISP * TERMS * 24
    mats = pl.pallas_call(
        prep_kernel,
        grid=(2,),
        out_shape=tuple(sds(2, PAIRS, ZPAD, n) for n in (256, LANES, LANES)),
        in_specs=[
            pl.BlockSpec((1, DISP, 3, TERMS, 400), lambda l: (l, 0, 0, 0, 0)),
            SM,
            const((24, 400)),
            const((24, 400)),
            const((2, 400, 128)),
            const((3, 128, LANES)),
        ],
        out_specs=tuple(
            pl.BlockSpec((1, PAIRS, ZPAD, n), lambda l: (l, 0, 0, 0)) for n in (256, LANES, LANES)
        ),
        scratch_shapes=[pltpu.VMEM((rows, 400), F32)] * 3,
        compiler_params=_params(),
        cost_estimate=COST,
        name="prep",
    )(ob.transpose(0, 1, 3, 2, 4), ranks, jnp.asarray(c["ci"]), jnp.asarray(c["ca"]), _onehot(c["folds"]), _onehot(c["wide"]))
    wall = jnp.concatenate([wall, traded(wall, "gz", 2)], axis=0)
    wall, *mats = lax.optimization_barrier((wall, *mats))
    wall = [wall, local(traded(wall, "gz", 4))]

    coarse = pl.pallas_call(
        coarse_kernel,
        out_shape=sds(8, 24, 128),
        in_specs=[VM, SM, SM, AN, AN, AN, VM],
        out_specs=VM,
        scratch_shapes=[
            *level_scratch(1),
            pltpu.VMEM((4 * DISP, 8, 1280), F32),
            pltpu.VMEM((80, LANES), F32),
            pltpu.VMEM((LANES, LANES), BF16),
        ],
        compiler_params=_params(),
        cost_estimate=COST,
        name="coarse",
    )(local(corners), pp, ranks, *mats, lanes)
    middle = pl.pallas_call(
        middle_kernel,
        out_shape=(sds(40, LANES),) * 4,
        in_specs=[*[VM] * 2, SM, AN, AN, AN, VM],
        out_specs=(VM,) * 4,
        scratch_shapes=[
            *level_scratch(2),
            pltpu.VMEM((8, 1, 640), F32),
            pltpu.VMEM((640, LANES), BF16),
        ],
        compiler_params=_params(),
        cost_estimate=COST,
        name="middle",
    )(*wall, ranks, *mats, _onehot(c["po"]))
    coarse = swap(coarse, "gz")
    middle = [middle[0]] + [local(shifted(m, "gy", k + 1)) for k, m in enumerate(middle[1:])]
    return pl.pallas_call(
        final_kernel,
        out_shape=sds(16, 1000),
        in_specs=[VM] * 9,
        out_specs=VM,
        compiler_params=_params(),
        name="final",
    )(*middle, local(coarse), lanes, _pair(c["ht"]), _pair(c["hyt"]), _onehot(c["rt"]))


def solution(mesh):
    in_specs = (
        P(("gx", "gy", "gz"), None),
        P(),
        P(),
        P(("gx", "gy", "gz"), None, None),
        P(("gx", "gy", "gz"), None),
        P(("gx", "gy"), None),
        P(("gx", "gy"), None),
    )
    out_specs = P(("gx", "gy", "gz"), None)
    return jax.shard_map(
        on_device, mesh=mesh, in_specs=in_specs, out_specs=out_specs, check_vma=False
    )
```
